32 devices in a mesh: groups: 2 (over y), row: 16 (over z, x, core).
Axes of the slice: x: 2, y: 2, z: 4, core: 2. Of those that a mesh axis runs over, the one named last changes fastest.
Arguments:
- raw_samples: bfloat16 [8, 1536, 1280], P('groups', 'row'), parts along dimension 0, may hold values from -64 to 64, as said below
- partner: int32 [32, 3], P(('groups', 'row')), parts along dimension 0, may hold values from -1 to 15, as said below
- counts: int32 [32, 3], P(('groups', 'row')), parts along dimension 0, may hold values from 1 to 4
Outputs:
- correlations: bfloat16 [32, 3, 80, 80, 128], P(('groups', 'row')), parts along dimension 0
The draws below stay inside these ranges and needn't reach their ends.
There are 2 independent parts, one for each index of `groups`. The reference program is written for one: setup_inputs(seed, part) draws one part's arguments, and reference() takes and returns one part's arrays. A program takes and returns all parts, laid end to end along the dimension named above; each array names one. Nothing has to cross between parts.
Inputs may be any that keep to these rules, and one draw needn't show every extreme that they name: `raw_samples`: strain values of each channel and segment at their own scale. `partner`: slot 0 of row i holds i; slots 1 to r hold i + 1 to i + r for some r of 0 to 2 with i + r < 16; the other slots hold -1. Some row has r = 2. A tile stacks its first counts segments.
All inputs are finite; a program needn't handle non-finite values.
Results may differ from the reference program's by a relative error of at most 0.0075.
Values may be sent and summed in bfloat16 or wider, within the bound.
A program may use at most 128 MiB of HBM per device.

```python
import math
import jax
import jax.numpy as jnp
from jax import lax

SEG = 4
SAMPLES = 1536
BINS = 192
FIRST_BIN = 5
LAGS = 128
LAG_STEP = 4
BLOCK = 80
BAND = 2
SLOTS = 3
BLOCKS = 16
CHANNELS = 1280


def draw_raw_samples(key, part):
    first_key, second_key, third_key = jax.random.split(jax.random.fold_in(key, 11), 3)
    shape = (SEG, SAMPLES, CHANNELS)
    seg_scale = jnp.exp(jax.random.uniform(second_key, (SEG, 1, 1), jnp.float32, math.log(0.5), math.log(2.0)))
    chan_scale = jnp.exp(jax.random.uniform(first_key, (1, 1, CHANNELS), jnp.float32, math.log(0.3), math.log(3.0)))
    values = jnp.clip(jax.random.normal(third_key, shape, jnp.float32), -4.0, 4.0)
    return (values * chan_scale * seg_scale).astype(jnp.bfloat16)


def draw_partner(key, part):
    first_key, second_key = jax.random.split(jax.random.fold_in(key, 23))
    block_rows = jnp.arange(BLOCKS, dtype=jnp.int32)
    reaches = jax.random.randint(first_key, (BLOCKS,), 0, BAND + 1, dtype=jnp.int32)
    forced = jax.random.randint(second_key, (), 0, BLOCKS - BAND, dtype=jnp.int32)
    reaches = jnp.where(block_rows == forced, BAND, reaches)
    reaches = jnp.minimum(reaches, BLOCKS - 1 - block_rows)
    offsets = jnp.arange(SLOTS, dtype=jnp.int32)
    listed = jnp.where(offsets[None, :] <= reaches[:, None], block_rows[:, None] + offsets[None, :], -1)
    return listed.astype(jnp.int32)


def with_ends(entries, own_key, low, largest):
    spot = [jax.random.randint(jax.random.fold_in(own_key, axis), (), 0, length) for axis, length in enumerate(entries.shape)]
    main_axis = entries.shape.index(max(entries.shape))
    beside = spot[:main_axis] + [(spot[main_axis] + 1) % entries.shape[main_axis]] + spot[main_axis + 1:]
    return entries.at[tuple(spot)].set(low).at[tuple(beside)].set(largest)


def setup_inputs(seed: int = 0, part: int = 0) -> dict:
    splits = jax.random.split(jax.random.key(seed), 4)
    part_keys = jax.random.split(jax.random.fold_in(splits[3], part), 4)
    raw_samples = draw_raw_samples(jax.random.fold_in(jax.random.fold_in(splits[3], part), 71), part)
    partner = draw_partner(jax.random.fold_in(jax.random.fold_in(splits[3], part), 71), part)
    counts = with_ends(jax.random.randint(part_keys[2], (BLOCKS, SLOTS), 1, SEG + 1), jax.random.fold_in(part_keys[2], 1), 1, SEG).astype(jnp.int32)
    return dict(raw_samples=raw_samples, partner=partner, counts=counts)


def forward_table(length, first_bin, bin_count):
    sample_idx = jnp.arange(length, dtype=jnp.int32)[:, None]
    bin_index = first_bin + jnp.arange(bin_count, dtype=jnp.int32)[None, :]
    angles = 2.0 * math.pi / length * (sample_idx * bin_index % length).astype(jnp.float32)
    return jnp.concatenate([jnp.cos(angles), -jnp.sin(angles)], axis=1).astype(jnp.bfloat16)

def lag_table(length, first_bin, bin_count, lag_count, lag_step):
    bin_index = first_bin + jnp.arange(bin_count, dtype=jnp.int32)[:, None]
    delays = lag_step * (jnp.arange(lag_count, dtype=jnp.int32)[None, :] - lag_count // 2)
    angles = 2.0 * math.pi / length * (bin_index * delays % length).astype(jnp.float32)
    return jnp.concatenate([jnp.cos(angles), -jnp.sin(angles)], axis=0).astype(jnp.bfloat16)

def tile_lags(left_block, right_block, seg_count, lag_matrix):
    segments, block_width, doubled = left_block.shape
    bin_count = doubled // 2
    keep_mask = (jnp.arange(segments, dtype=jnp.int32) < seg_count).astype(jnp.float32)
    left_block = left_block.astype(jnp.float32) * keep_mask[:, None, None]
    right_block = right_block.astype(jnp.float32)
    left_parts = jnp.stack([left_block[..., :bin_count], left_block[..., bin_count:]], axis=1)
    right_parts = jnp.stack([right_block[..., :bin_count], right_block[..., bin_count:]], axis=1)
    turned = jnp.stack([right_block[..., bin_count:], -right_block[..., :bin_count]], axis=1)
    real_sum = jnp.einsum('spaf,spbf->abf', left_parts, right_parts, precision=lax.Precision.HIGHEST)
    imag_sum = jnp.einsum('spaf,spbf->abf', left_parts, turned, precision=lax.Precision.HIGHEST)
    scaling = lax.rsqrt(seg_count.astype(jnp.float32))
    stacked = (jnp.concatenate([real_sum, imag_sum], axis=-1) * scaling).astype(jnp.bfloat16)
    lagged = jnp.dot(stacked.reshape(block_width * block_width, doubled), lag_matrix, preferred_element_type=jnp.float32)
    return lagged.reshape(block_width, block_width, -1) * (1.0 / math.sqrt(bin_count))

def reference(raw_samples, partner, counts):
    segments, length, channels = raw_samples.shape
    blocks = channels // BLOCK
    dft_table = forward_table(length, FIRST_BIN, BINS)
    spectra = jnp.einsum('slc,lf->scf', raw_samples.astype(jnp.float32), dft_table.astype(jnp.float32), precision=lax.Precision.HIGHEST)
    energy = 2.0 * lax.optimization_barrier(jnp.mean(spectra * spectra, axis=-1, keepdims=True))
    white = (spectra * lax.rsqrt(energy + 1e-06)).astype(jnp.bfloat16)
    lag_matrix = lag_table(length, FIRST_BIN, BINS, LAGS, LAG_STEP)
    above_diag = jnp.arange(BLOCK)[:, None] < jnp.arange(BLOCK)[None, :]

    def one_tile(tile_index):
        block_row = tile_index // SLOTS
        offset = tile_index % SLOTS
        partner_block = partner[block_row, offset]
        seg_count = counts[block_row, offset]
        left_block = lax.dynamic_slice_in_dim(white, (block_row * BLOCK).astype(jnp.int32), BLOCK, 1)
        right_block = lax.dynamic_slice_in_dim(white, (jnp.maximum(partner_block, 0) * BLOCK).astype(jnp.int32), BLOCK, 1)
        lagged = tile_lags(left_block, right_block, seg_count, lag_matrix)
        keeping = jnp.where(partner_block == block_row, above_diag, partner_block >= 0)
        return jnp.where(keeping[:, :, None], lagged, 0.0).astype(jnp.bfloat16)
    tiles = lax.map(one_tile, jnp.arange(blocks * SLOTS, dtype=jnp.int32))
    return tiles.reshape(blocks, SLOTS, BLOCK, BLOCK, LAGS)
```

```python
import functools
import math

import jax
import jax.numpy as jnp
import numpy as np
from jax import lax
from jax.experimental import pallas as pl
from jax.experimental.pallas import tpu as pltpu
from jax.sharding import PartitionSpec as P

SAMPLES = 1536
BINS = 192
FIRST_BIN = 5
LAGS = 128
LAG_STEP = 4
SLOTS = 3
WIDTH = 2 * BINS
HALF = BINS - 128
PARTS = WIDTH // 128
GROUP = 8
ROWS_PER_STEP = 16
MESH = pl.DeviceIdType.MESH


def bin_order():
    bins = np.concatenate([np.arange(BINS), np.arange(128, BINS), np.arange(128)])
    imag = np.arange(WIDTH) >= BINS
    return bins, imag


def angle(product):
    return np.float32(2.0 * math.pi / SAMPLES) * (product % SAMPLES).astype(np.float32)


def forward_table():
    bins, imag = bin_order()
    angles = angle(np.arange(SAMPLES)[:, None] * (FIRST_BIN + bins)[None, :])
    return jnp.asarray(np.where(imag[None, :], -np.sin(angles), np.cos(angles)).astype(np.float32)).astype(jnp.bfloat16)


def lag_tables():
    bins, imag = bin_order()
    delays = LAG_STEP * (np.arange(LAGS) - LAGS // 2)
    angles = angle(delays[:, None] * (FIRST_BIN + bins[:256])[None, :])
    straight = np.cos(angles).astype(np.float32)
    crossed = np.where(imag[None, :256], -np.sin(angles), np.sin(angles)).astype(np.float32)
    tables = np.stack([straight[:, :128], straight[:, 128:], crossed[:, :128], crossed[:, 128:]])
    return jnp.asarray(tables).astype(jnp.bfloat16)


def tile_plan(segments, local):
    lanes = segments * local
    width = 128 if lanes % 128 == 0 else lanes
    tiles = lanes // width
    parts = [(s, t) for s in range(segments) for t in range(PARTS)]
    pieces, stages, done, used = [], [], 0, 0
    for j in range(tiles):
        row = []
        for s in range(segments):
            lo, hi = max(s * local, j * width), min((s + 1) * local, (j + 1) * width)
            if lo < hi:
                row.append((s, lo - j * width, hi - j * width, lo - s * local))
        pieces.append(row)
        whole = (j + 1) * width // local
        if whole > done:
            ready = whole * PARTS
            ready -= ready % 2 if j < tiles - 1 else 0
            stages.append((j, list(range(done, whole)), parts[used:ready]))
            done, used = whole, ready
    return width, pieces, stages


def turned_pair(rows, mid, lag, parts, base, first):
    halves = []
    for k in range(2):
        i = first + k
        columns = []
        for s, t in parts:
            if t == 1:
                x, y, c = rows[s, 1, pl.ds(base, GROUP), :], mid[s, pl.ds(base, GROUP), :], 1
            else:
                x, y, c = rows[s, t, pl.ds(base, GROUP), :], rows[s, 2 - t, pl.ds(base, GROUP), :], 0
            x, y = (jnp.broadcast_to(v[i:i + 1], (16, 128)).astype(jnp.bfloat16) for v in (x, y))
            column = []
            for m in range(0, LAGS, 16):
                straight, crossed = x * lag[c, m:m + 16], y * lag[c + 2, m:m + 16]
                column.append(straight - crossed if t == 2 else straight + crossed)
            columns.append(jnp.concatenate(column, axis=0))
        halves.append(jnp.concatenate(columns, axis=1))
    return jnp.concatenate(halves, axis=0)


def turn_rows(rows, mid, s, value):
    for t in range(PARTS):
        rows[s, t] = value[:, t * 128:(t + 1) * 128]
    mid[s] = pltpu.roll(value[:, 128:256], HALF, 1)


def lag_dot(right, turned, parts):
    left = jnp.concatenate([right[t] for t in range(parts)], axis=1)
    return lax.dot_general(left, turned, (((1,), (1,)), ((), ())), preferred_element_type=jnp.float32)


def slot_scale(partner, counts, slot):
    live = (partner[0, slot] >= 0).astype(jnp.float32)
    count = jnp.full((8, LAGS), counts[0, slot].astype(jnp.float32), jnp.float32)
    return (lax.rsqrt(count) * (live * (1.0 / math.sqrt(BINS))))[0:1]


def masked(source, s, t, counts, slot):
    return (source[s, t].astype(jnp.float32) * (s < counts[0, slot]).astype(jnp.float32)).astype(jnp.bfloat16)


def exchange_kernel(n, width, pieces, stages, raw, table_hbm, lag_hbm, counts_hbm, own, near, far, acc,
                    raw_v, table, lag, counts, turned, landed, spec, right, rows, mid, load_sem, send_sem, recv_sem, pass_send, pass_recv):
    me = lax.axis_index("row")
    segments, _, block, _ = own.shape
    tiles = len(pieces)
    channels = turned.shape[1]
    barrier = pltpu.get_barrier_semaphore()

    def ahead(k):
        return lax.rem(me + k, n)

    @pl.loop(1, n)
    def _(k):
        pl.semaphore_signal(barrier, inc=1, device_id={"row": ahead(k)}, device_id_type=MESH)

    loads = [pltpu.make_async_copy(raw.at[j], raw_v.at[j], load_sem.at[j]) for j in range(tiles)]
    more = [pltpu.make_async_copy(source, place, load_sem.at[tiles + i]) for i, (source, place) in enumerate(
        ((counts_hbm, counts), (table_hbm, table), (lag_hbm, lag)))]
    for copy in loads + more:
        copy.start()

    def tile_copy(j, k):
        target = ahead(k)
        return pltpu.make_async_remote_copy(
            src_ref=turned.at[j, pl.ds(pl.multiple_of(target * block, 16), block)],
            dst_ref=landed.at[j, me],
            send_sem=send_sem.at[j, k],
            recv_sem=recv_sem.at[j, k],
            device_id={"row": target},
            device_id_type=MESH,
        )

    def send(j, lo, hi):
        @pl.loop(lo, hi)
        def _(k):
            tile_copy(j, k).start()

    half = n // 2

    def send_next(j):
        if tiles > 2 and j < 2:
            for i in range(2, tiles):
                send(i, *((1, half), (half, n))[j])

    for j in range(tiles):
        loads[j].wait()

        @pl.loop(0, channels // 128)
        def _(i):
            part = pl.ds(pl.multiple_of(i * 128, 128), 128)
            turned[j, part, :] = raw_v[j, :, part].T

        if j == 0:
            pl.semaphore_wait(barrier, n - 1)
        if j < 2:
            send(j, 1, n)

    for copy in more:
        copy.wait()

    def transform(j, source, x, fresh):
        for s, lo, hi, t in pieces[j]:
            part = jnp.dot(x[:, lo:hi], table[source, t:t + hi - lo], preferred_element_type=jnp.float32)
            spec[s] = part if fresh and t == 0 else spec[s] + part

    def spectra_first(j):
        transform(j, me, turned[j, pl.ds(pl.multiple_of(me * block, 16), block), :], True)
        spectra_part(j, 1, half)

    def spectra_part(j, lo, hi):
        @pl.loop(lo, hi)
        def _(k):
            tile_copy(j, k).wait_recv()
            source = lax.rem(me + n - k, n)
            transform(j, source, landed[j, source], False)

    def whiten(segs):
        for s in segs:
            value = spec[s]
            energy = 2.0 * jnp.mean(value * value, axis=-1, keepdims=True)
            white = (value * lax.rsqrt(energy + 1e-06)).astype(jnp.bfloat16)
            for t in range(PARTS):
                own[s, t] = white[:, t * 128:(t + 1) * 128]
            turn_rows(rows, mid, s, white.astype(jnp.float32))

    odd = lax.rem(me, 2) == 1
    senders = (me >= 1, jnp.logical_and(odd, me >= 2), jnp.logical_and(odd, me + 1 < n))

    def pass_copy(stage, segs, kind):
        part = pl.ds(segs[0], len(segs))
        source, place, back = ((own, near, 1), (own, far, 2), (near, far, 1))[kind]
        return pltpu.make_async_remote_copy(
            src_ref=source.at[part], dst_ref=place.at[part], send_sem=pass_send.at[stage, kind],
            recv_sem=pass_recv.at[stage, min(kind, 1)], device_id={"row": ahead(n - back)}, device_id_type=MESH,
        )

    def pass_start(stage, segs):
        for kind in range(2):
            @pl.when(senders[kind])
            def _():
                pass_copy(stage, segs, kind).start()

    def pass_near(stage, segs):
        @pl.when(me + 1 < n)
        def _():
            pass_copy(stage, segs, 0).wait_recv()

        @pl.when(senders[2])
        def _():
            pass_copy(stage, segs, 2).start()

    def pass_far(stage, segs):
        @pl.when(me + 2 < n)
        def _():
            pass_copy(stage, segs, 1).wait_recv()

    def pass_sent(stage, segs):
        for kind, sends in enumerate(senders):
            @pl.when(sends)
            def _():
                pass_copy(stage, segs, kind).wait_send()

    for i, place in enumerate((near, far)):
        @pl.when(me + i + 1 >= n)
        def _():
            place[...] = jnp.zeros_like(place)

    pairs = GROUP // 2

    def take_rows(parts):
        for slot, source in enumerate((own, near, far)):
            for at, (s, t) in enumerate(parts):
                right[at, slot * block:(slot + 1) * block] = masked(source, s, t, counts, slot)

    def correlate_rows(parts, total, lo, hi):
        @pl.loop(lo // GROUP, hi // GROUP)
        def _(g):
            base = pl.multiple_of(g * GROUP, GROUP)
            for p in range(pairs):
                result = lag_dot(right, turned_pair(rows, mid, lag, parts, base, 2 * p), len(parts))
                for k in range(2):
                    a = base + 2 * p + k
                    for slot in range(SLOTS):
                        part = result[slot * block:(slot + 1) * block, k * LAGS:(k + 1) * LAGS]
                        acc[slot, a] = acc[slot, a] + part if total else part

    last = len(stages) - 1
    middle = block // 2 // GROUP * GROUP
    if not last:
        acc[...] = jnp.zeros_like(acc)

    def spectra(j):
        spectra_first(j)
        spectra_part(j, half, n)

    def arrive(stage):
        segs = stages[stage][1]
        pass_near(stage, segs)
        pass_far(stage, segs)

    for stage, (j, segs, parts) in enumerate(stages):
        for i in range(stages[stage - 1][0] + 1 if stage else 0, j + 1):
            spectra(i)
        whiten(segs)
        pass_start(stage, segs)
        send_next(j)
        if 0 < stage:
            arrive(stage - 1)
            take_rows(stages[stage - 1][2])
            correlate_rows(stages[stage - 1][2], stage > 1, 0, middle)
            if stage == last:
                pass_near(stage, segs)
            correlate_rows(stages[stage - 1][2], stage > 1, middle, block)
    if not last:
        pass_near(last, stages[last][1])
    for j in range(tiles):
        @pl.loop(1, n)
        def _(k):
            tile_copy(j, k).wait_send()
    pass_far(last, stages[last][1])
    for stage, (_, segs, _) in enumerate(stages):
        pass_sent(stage, segs)


def exchange(raw_samples, counts, width, pieces, stages):
    n = lax.axis_size("row")
    segments, local, channels = raw_samples.shape
    block = channels // n
    tiles = len(pieces)
    parts = max(len(parts) for _, _, parts in stages)
    white = jax.ShapeDtypeStruct((segments, PARTS, block, 128), jnp.bfloat16)
    vmem = pl.BlockSpec(memory_space=pltpu.VMEM)
    hbm = pl.BlockSpec(memory_space=pltpu.HBM)
    inputs = (raw_samples.reshape(tiles, width, channels), forward_table().reshape(n, local, WIDTH), lag_tables(), counts)
    return pl.pallas_call(
        functools.partial(exchange_kernel, n, width, pieces, stages),
        out_shape=(white,) * 3 + (jax.ShapeDtypeStruct((SLOTS, block, block, LAGS), jnp.float32),),
        in_specs=[hbm] * 4,
        out_specs=(vmem,) * 4,
        scratch_shapes=[
            pltpu.VMEM((tiles, width, channels), jnp.bfloat16),
            pltpu.VMEM((n, local, WIDTH), jnp.bfloat16),
            pltpu.VMEM((4, LAGS, 128), jnp.bfloat16),
            pltpu.SMEM((1, SLOTS), jnp.int32),
            pltpu.VMEM((tiles, channels, width), jnp.bfloat16),
            pltpu.VMEM((tiles, n, block, width), jnp.bfloat16),
            pltpu.VMEM((segments, block, WIDTH), jnp.float32),
            pltpu.VMEM((parts, SLOTS * block, 128), jnp.bfloat16),
            pltpu.VMEM((segments, PARTS, block, 128), jnp.float32),
            pltpu.VMEM((segments, block, 128), jnp.float32),
            pltpu.SemaphoreType.DMA((tiles + 3,)),
            pltpu.SemaphoreType.DMA((tiles, n)),
            pltpu.SemaphoreType.DMA((tiles, n)),
            pltpu.SemaphoreType.DMA((len(stages), 3)),
            pltpu.SemaphoreType.DMA((len(stages), 2)),
        ],
        compiler_params=pltpu.CompilerParams(collective_id=0, has_side_effects=True, vmem_limit_bytes=20_000_000),
        cost_estimate=pl.CostEstimate(flops=20_000_000_000, bytes_accessed=4_000_000, transcendentals=0),
        name="exchange",
    )(*(pltpu.with_memory_space_constraint(x, pltpu.HBM) for x in inputs))


def correlate_kernel(parts, partner, counts, own, near, far, acc, lag_in, out, right, rows, mid, lag):
    block = own.shape[2]
    step = pl.program_id(0)
    first = pl.multiple_of(step * ROWS_PER_STEP, ROWS_PER_STEP)

    @pl.when(step == 0)
    def _():
        for slot, source in enumerate((own, near, far)):
            for at, (s, t) in enumerate(parts):
                right[at, slot * block:(slot + 1) * block] = masked(source, s, t, counts, slot)
        for s in sorted({s for s, _ in parts}):
            turn_rows(rows, mid, s, jnp.concatenate([own[s, t].astype(jnp.float32) for t in range(PARTS)], axis=1))
        lag[...] = lag_in[...]

    scales = [slot_scale(partner, counts, slot) for slot in range(SLOTS)]
    pairs = ROWS_PER_STEP // 2
    for pair in range(pairs):
        base = pl.multiple_of(first + 2 * pair // GROUP * GROUP, GROUP)
        result = lag_dot(right, turned_pair(rows, mid, lag, parts, base, 2 * pair % GROUP), len(parts))
        for k in range(2):
            i = 2 * pair + k
            a = first + i
            for slot in range(SLOTS):
                part = result[slot * block:(slot + 1) * block, k * LAGS:(k + 1) * LAGS]
                part = (acc[slot, a] + part) * scales[slot]
                if slot == 0:
                    part = jnp.where(lax.broadcasted_iota(jnp.int32, part.shape, 0) > a, part, 0.0)
                out[0, slot, i] = part.astype(jnp.bfloat16)


def correlate(parts, partner, counts, own, near, far, acc):
    segments, _, block, _ = own.shape
    vmem = pl.BlockSpec(memory_space=pltpu.VMEM)
    return pl.pallas_call(
        functools.partial(correlate_kernel, parts),
        grid_spec=pltpu.PrefetchScalarGridSpec(
            num_scalar_prefetch=0,
            grid=(block // ROWS_PER_STEP,),
            in_specs=[pl.BlockSpec(memory_space=pltpu.SMEM)] * 2 + [vmem] * 5,
            out_specs=pl.BlockSpec((1, SLOTS, ROWS_PER_STEP, block, LAGS), lambda i, *_: (0, 0, i, 0, 0)),
            scratch_shapes=[
                pltpu.VMEM((len(parts), SLOTS * block, 128), jnp.bfloat16),
                pltpu.VMEM((segments, PARTS, block, 128), jnp.float32),
                pltpu.VMEM((segments, block, 128), jnp.float32),
                pltpu.VMEM((4, LAGS, 128), jnp.bfloat16),
            ],
        ),
        out_shape=jax.ShapeDtypeStruct((1, SLOTS, block, block, LAGS), jnp.bfloat16),
        cost_estimate=pl.CostEstimate(
            flops=6 * block * block * LAGS * len(parts) * 128, bytes_accessed=6_000_000, transcendentals=0),
        compiler_params=pltpu.CompilerParams(vmem_limit_bytes=10 * 2**20),
        name="correlate",
    )(partner, counts, own, near, far, acc, lag_tables())


def on_device(raw_samples, partner, counts):
    width, pieces, stages = tile_plan(raw_samples.shape[0], raw_samples.shape[1])
    own, near, far, acc = exchange(raw_samples, counts, width, pieces, stages)
    return correlate(stages[-1][2], partner, counts, own, near, far, acc)


def solution(mesh):
    return jax.shard_map(
        on_device,
        mesh=mesh,
        in_specs=(P("groups", "row", None), P(("groups", "row"), None), P(("groups", "row"), None)),
        out_specs=P(("groups", "row"), None, None, None, None),
        check_vma=False,
    )
```

```python
import functools
import math

import jax
import jax.numpy as jnp
import numpy as np
from jax import lax
from jax.experimental import pallas as pl
from jax.experimental.pallas import tpu as pltpu
from jax.sharding import PartitionSpec as P

SAMPLES = 1536
BINS = 192
FIRST_BIN = 5
LAGS = 128
LAG_STEP = 4
SLOTS = 3
WIDTH = 2 * BINS
HALF = BINS - 128
PARTS = WIDTH // 128
GROUP = 8
RUN = 40
MESH = pl.DeviceIdType.MESH


def bin_order():
    bins = np.concatenate([np.arange(BINS), np.arange(128, BINS), np.arange(128)])
    imag = np.arange(WIDTH) >= BINS
    return bins, imag


def angle(product):
    return np.float32(2.0 * math.pi / SAMPLES) * (product % SAMPLES).astype(np.float32)


def forward_table():
    bins, imag = bin_order()
    angles = angle(np.arange(SAMPLES)[:, None] * (FIRST_BIN + bins)[None, :])
    return jnp.asarray(np.where(imag[None, :], -np.sin(angles), np.cos(angles)).astype(np.float32)).astype(jnp.bfloat16)


def lag_tables():
    bins, imag = bin_order()
    delays = LAG_STEP * (np.arange(LAGS) - LAGS // 2)
    angles = angle(delays[:, None] * (FIRST_BIN + bins[:256])[None, :])
    straight = np.cos(angles).astype(np.float32)
    crossed = np.where(imag[None, :256], -np.sin(angles), np.sin(angles)).astype(np.float32)
    tables = np.stack([straight[:, :128], straight[:, 128:], crossed[:, :128], crossed[:, 128:]])
    return jnp.asarray(tables).astype(jnp.bfloat16)


def tile_plan(segments, local):
    lanes = segments * local
    width = 128 if lanes % 128 == 0 else lanes
    tiles = lanes // width
    parts = [(s, t) for s in range(segments) for t in range(PARTS)]
    pieces, stages, done, used = [], [], 0, 0
    for j in range(tiles):
        row = []
        for s in range(segments):
            lo, hi = max(s * local, j * width), min((s + 1) * local, (j + 1) * width)
            if lo < hi:
                row.append((s, lo - j * width, hi - j * width, lo - s * local))
        pieces.append(row)
        whole = (j + 1) * width // local
        if whole > done:
            ready = whole * PARTS
            ready -= ready % 2 if j < tiles - 1 else 0
            stages.append((j, list(range(done, whole)), parts[used:ready]))
            done, used = whole, ready
    return width, pieces, stages


def turned_pair(rows, mid, lag, parts, base, first):
    halves = []
    for k in range(2):
        i = first + k
        columns = []
        for s, t in parts:
            if t == 1:
                x, y, c = rows[s, 1, pl.ds(base, GROUP), :], mid[s, pl.ds(base, GROUP), :], 1
            else:
                x, y, c = rows[s, t, pl.ds(base, GROUP), :], rows[s, 2 - t, pl.ds(base, GROUP), :], 0
            x, y = (jnp.broadcast_to(v[i:i + 1], (16, 128)).astype(jnp.bfloat16) for v in (x, y))
            column = []
            for m in range(0, LAGS, 16):
                straight, crossed = x * lag[c, m:m + 16], y * lag[c + 2, m:m + 16]
                column.append(straight - crossed if t == 2 else straight + crossed)
            columns.append(jnp.concatenate(column, axis=0))
        halves.append(jnp.concatenate(columns, axis=1))
    return jnp.concatenate(halves, axis=0)


def turn_rows(rows, mid, s, value):
    for t in range(PARTS):
        rows[s, t] = value[:, t * 128:(t + 1) * 128]
    mid[s] = pltpu.roll(value[:, 128:256], HALF, 1)


def lag_dot(right, turned, parts):
    left = jnp.concatenate([right[t] for t in range(parts)], axis=1)
    return lax.dot_general(left, turned, (((1,), (1,)), ((), ())), preferred_element_type=jnp.float32)


def slot_scale(partner, counts, slot):
    live = (partner[0, slot] >= 0).astype(jnp.float32)
    count = jnp.full((8, LAGS), counts[0, slot].astype(jnp.float32), jnp.float32)
    return (lax.rsqrt(count) * (live * (1.0 / math.sqrt(BINS))))[0:1]


def masked(source, s, t, counts, slot):
    return (source[s, t].astype(jnp.float32) * (s < counts[0, slot]).astype(jnp.float32)).astype(jnp.bfloat16)


def exchange_kernel(n, width, pieces, stages, raw, table_hbm, lag_hbm, counts_hbm, own, near, far, acc,
                    raw_v, table, lag, counts, turned, landed, spec, right, rows, mid, load_sem, send_sem, recv_sem, pass_send, pass_recv):
    me = lax.axis_index("row")
    segments, _, block, _ = own.shape
    tiles = len(pieces)
    channels = turned.shape[1]
    barrier = pltpu.get_barrier_semaphore()

    def ahead(k):
        return lax.rem(me + k, n)

    @pl.loop(1, n)
    def _(k):
        pl.semaphore_signal(barrier, inc=1, device_id={"row": ahead(k)}, device_id_type=MESH)

    loads = [pltpu.make_async_copy(raw.at[j], raw_v.at[j], load_sem.at[j]) for j in range(tiles)]
    more = [pltpu.make_async_copy(source, place, load_sem.at[tiles + i]) for i, (source, place) in enumerate(
        ((counts_hbm, counts), (table_hbm, table), (lag_hbm, lag)))]
    for copy in loads + more:
        copy.start()

    def tile_copy(j, k):
        target = ahead(k)
        return pltpu.make_async_remote_copy(
            src_ref=turned.at[j, pl.ds(pl.multiple_of(target * block, 16), block)],
            dst_ref=landed.at[j, me],
            send_sem=send_sem.at[j, k],
            recv_sem=recv_sem.at[j, k],
            device_id={"row": target},
            device_id_type=MESH,
        )

    def send(j, lo, hi):
        @pl.loop(lo, hi)
        def _(k):
            tile_copy(j, k).start()

    half = n // 2

    def send_next(j):
        if tiles > 2 and j < 2:
            for i in range(2, tiles):
                send(i, *((1, half), (half, n))[j])

    for j in range(tiles):
        loads[j].wait()

        @pl.loop(0, channels // 128)
        def _(i):
            part = pl.ds(pl.multiple_of(i * 128, 128), 128)
            turned[j, part, :] = raw_v[j, :, part].T

        if j == 0:
            pl.semaphore_wait(barrier, n - 1)
        if j < 2:
            send(j, 1, n)

    for copy in more:
        copy.wait()

    def transform(j, source, x, fresh):
        for s, lo, hi, t in pieces[j]:
            part = jnp.dot(x[:, lo:hi], table[source, t:t + hi - lo], preferred_element_type=jnp.float32)
            spec[s] = part if fresh and t == 0 else spec[s] + part

    def spectra_first(j):
        transform(j, me, turned[j, pl.ds(pl.multiple_of(me * block, 16), block), :], True)
        spectra_part(j, 1, half)

    def spectra_part(j, lo, hi):
        @pl.loop(lo, hi)
        def _(k):
            tile_copy(j, k).wait_recv()
            source = lax.rem(me + n - k, n)
            transform(j, source, landed[j, source], False)

    def whiten(segs):
        for s in segs:
            value = spec[s]
            energy = 2.0 * jnp.mean(value * value, axis=-1, keepdims=True)
            white = (value * lax.rsqrt(energy + 1e-06)).astype(jnp.bfloat16)
            for t in range(PARTS):
                own[s, t] = white[:, t * 128:(t + 1) * 128]
            turn_rows(rows, mid, s, white.astype(jnp.float32))

    odd = lax.rem(me, 2) == 1
    senders = (me >= 1, jnp.logical_and(odd, me >= 2), jnp.logical_and(odd, me + 1 < n))

    def pass_copy(stage, segs, kind):
        part = pl.ds(segs[0], len(segs))
        source, place, back = ((own, near, 1), (own, far, 2), (near, far, 1))[kind]
        return pltpu.make_async_remote_copy(
            src_ref=source.at[part], dst_ref=place.at[part], send_sem=pass_send.at[stage, kind],
            recv_sem=pass_recv.at[stage, min(kind, 1)], device_id={"row": ahead(n - back)}, device_id_type=MESH,
        )

    def pass_start(stage, segs):
        for kind in range(2):
            @pl.when(senders[kind])
            def _():
                pass_copy(stage, segs, kind).start()

    def pass_near(stage, segs):
        @pl.when(me + 1 < n)
        def _():
            pass_copy(stage, segs, 0).wait_recv()

        @pl.when(senders[2])
        def _():
            pass_copy(stage, segs, 2).start()

    def pass_far(stage, segs):
        @pl.when(me + 2 < n)
        def _():
            pass_copy(stage, segs, 1).wait_recv()

    def pass_sent(stage, segs):
        for kind, sends in enumerate(senders):
            @pl.when(sends)
            def _():
                pass_copy(stage, segs, kind).wait_send()

    for i, place in enumerate((near, far)):
        @pl.when(me + i + 1 >= n)
        def _():
            place[...] = jnp.zeros_like(place)


    def take_rows(parts):
        for slot, source in enumerate((own, near, far)):
            for at, (s, t) in enumerate(parts):
                right[at, slot * block:(slot + 1) * block] = masked(source, s, t, counts, slot)

    def correlate_rows(parts, total, lo, hi):
        @pl.loop(0, (hi - lo) // RUN)
        def _(g):
            base = pl.multiple_of(lo + g * RUN, GROUP)
            for i in range(0, RUN, 2):
                result = lag_dot(right, turned_pair(rows, mid, lag, parts, base + i // GROUP * GROUP, i % GROUP), len(parts))
                for k in range(2):
                    a = base + i + k
                    for slot in range(SLOTS):
                        part = result[slot * block:(slot + 1) * block, k * LAGS:(k + 1) * LAGS]
                        acc[slot, a] = acc[slot, a] + part if total else part

    last = len(stages) - 1
    middle = block // 2 // RUN * RUN
    if not last:
        acc[...] = jnp.zeros_like(acc)

    def spectra(j):
        spectra_first(j)
        spectra_part(j, half, n)

    def arrive(stage):
        segs = stages[stage][1]
        pass_near(stage, segs)
        pass_far(stage, segs)

    for stage, (j, segs, parts) in enumerate(stages):
        for i in range(stages[stage - 1][0] + 1 if stage else 0, j + 1):
            spectra(i)
        whiten(segs)
        pass_start(stage, segs)
        send_next(j)
        if 0 < stage:
            arrive(stage - 1)
            take_rows(stages[stage - 1][2])
            correlate_rows(stages[stage - 1][2], stage > 1, 0, middle)
            if stage == last:
                pass_near(stage, segs)
            correlate_rows(stages[stage - 1][2], stage > 1, middle, block)
    if not last:
        pass_near(last, stages[last][1])
    for j in range(tiles):
        @pl.loop(1, n)
        def _(k):
            tile_copy(j, k).wait_send()
    pass_far(last, stages[last][1])
    for stage, (_, segs, _) in enumerate(stages):
        pass_sent(stage, segs)


def exchange(raw_samples, counts, width, pieces, stages):
    n = lax.axis_size("row")
    segments, local, channels = raw_samples.shape
    block = channels // n
    tiles = len(pieces)
    parts = max(len(parts) for _, _, parts in stages)
    white = jax.ShapeDtypeStruct((segments, PARTS, block, 128), jnp.bfloat16)
    vmem = pl.BlockSpec(memory_space=pltpu.VMEM)
    hbm = pl.BlockSpec(memory_space=pltpu.HBM)
    inputs = (raw_samples.reshape(tiles, width, channels), forward_table().reshape(n, local, WIDTH), lag_tables(), counts)
    return pl.pallas_call(
        functools.partial(exchange_kernel, n, width, pieces, stages),
        out_shape=(white,) * 3 + (jax.ShapeDtypeStruct((SLOTS, block, block, LAGS), jnp.float32),),
        in_specs=[hbm] * 4,
        out_specs=(vmem,) * 4,
        scratch_shapes=[
            pltpu.VMEM((tiles, width, channels), jnp.bfloat16),
            pltpu.VMEM((n, local, WIDTH), jnp.bfloat16),
            pltpu.VMEM((4, LAGS, 128), jnp.bfloat16),
            pltpu.SMEM((1, SLOTS), jnp.int32),
            pltpu.VMEM((tiles, channels, width), jnp.bfloat16),
            pltpu.VMEM((tiles, n, block, width), jnp.bfloat16),
            pltpu.VMEM((segments, block, WIDTH), jnp.float32),
            pltpu.VMEM((parts, SLOTS * block, 128), jnp.bfloat16),
            pltpu.VMEM((segments, PARTS, block, 128), jnp.float32),
            pltpu.VMEM((segments, block, 128), jnp.float32),
            pltpu.SemaphoreType.DMA((tiles + 3,)),
            pltpu.SemaphoreType.DMA((tiles, n)),
            pltpu.SemaphoreType.DMA((tiles, n)),
            pltpu.SemaphoreType.DMA((len(stages), 3)),
            pltpu.SemaphoreType.DMA((len(stages), 2)),
        ],
        compiler_params=pltpu.CompilerParams(collective_id=0, has_side_effects=True, vmem_limit_bytes=20_000_000),
        cost_estimate=pl.CostEstimate(flops=20_000_000_000, bytes_accessed=4_000_000, transcendentals=0),
        name="exchange",
    )(*(pltpu.with_memory_space_constraint(x, pltpu.HBM) for x in inputs))


def correlate_kernel(parts, partner, counts, own, near, far, acc, lag_in, out, staged, right, rows, mid, lag, out_sem):
    block = own.shape[2]
    for slot, source in enumerate((own, near, far)):
        for at, (s, t) in enumerate(parts):
            right[at, slot * block:(slot + 1) * block] = masked(source, s, t, counts, slot)
    for s in sorted({s for s, _ in parts}):
        turn_rows(rows, mid, s, jnp.concatenate([own[s, t].astype(jnp.float32) for t in range(PARTS)], axis=1))
    lag[...] = lag_in[...]
    scales = [slot_scale(partner, counts, slot) for slot in range(SLOTS)]

    def write(g):
        here = pl.ds(g * GROUP, GROUP)
        return pltpu.make_async_copy(staged.at[:, here], out.at[0, :, here], out_sem.at[g])

    for a in range(0, block, 2):
        result = lag_dot(right, turned_pair(rows, mid, lag, parts, a // GROUP * GROUP, a % GROUP), len(parts))
        for k in range(2):
            for slot in range(SLOTS):
                part = result[slot * block:(slot + 1) * block, k * LAGS:(k + 1) * LAGS]
                part = (acc[slot, a + k] + part) * scales[slot]
                if slot == 0:
                    part = jnp.where(lax.broadcasted_iota(jnp.int32, part.shape, 0) > a + k, part, 0.0)
                staged[slot, a + k] = part.astype(jnp.bfloat16)
        if (a + 2) % GROUP == 0:
            write(a // GROUP).start()
    for g in range(block // GROUP):
        write(g).wait()


def correlate(parts, partner, counts, own, near, far, acc):
    segments, _, block, _ = own.shape
    vmem = pl.BlockSpec(memory_space=pltpu.VMEM)
    return pl.pallas_call(
        functools.partial(correlate_kernel, parts),
        in_specs=[pl.BlockSpec(memory_space=pltpu.SMEM)] * 2 + [vmem] * 5,
        out_specs=pl.BlockSpec(memory_space=pltpu.HBM),
        scratch_shapes=[
            pltpu.VMEM((SLOTS, block, block, LAGS), jnp.bfloat16),
            pltpu.VMEM((len(parts), SLOTS * block, 128), jnp.bfloat16),
            pltpu.VMEM((segments, PARTS, block, 128), jnp.float32),
            pltpu.VMEM((segments, block, 128), jnp.float32),
            pltpu.VMEM((4, LAGS, 128), jnp.bfloat16),
            pltpu.SemaphoreType.DMA((block // GROUP,)),
        ],
        out_shape=jax.ShapeDtypeStruct((1, SLOTS, block, block, LAGS), jnp.bfloat16),
        cost_estimate=pl.CostEstimate(
            flops=6 * block * block * LAGS * len(parts) * 128, bytes_accessed=6_000_000, transcendentals=0),
        compiler_params=pltpu.CompilerParams(vmem_limit_bytes=15 * 2**20),
        name="correlate",
    )(partner, counts, own, near, far, acc, lag_tables())


def on_device(raw_samples, partner, counts):
    width, pieces, stages = tile_plan(raw_samples.shape[0], raw_samples.shape[1])
    own, near, far, acc = exchange(raw_samples, counts, width, pieces, stages)
    return correlate(stages[-1][2], partner, counts, own, near, far, acc)


def solution(mesh):
    return jax.shard_map(
        on_device,
        mesh=mesh,
        in_specs=(P("groups", "row", None), P(("groups", "row"), None), P(("groups", "row"), None)),
        out_specs=P(("groups", "row"), None, None, None, None),
        check_vma=False,
    )
```

```python
import functools
import math

import jax
import jax.numpy as jnp
import numpy as np
from jax import lax
from jax.experimental import pallas as pl
from jax.experimental.pallas import tpu as pltpu
from jax.sharding import PartitionSpec as P

SAMPLES = 1536
BINS = 192
FIRST_BIN = 5
LAGS = 128
LAG_STEP = 4
SLOTS = 3
WIDTH = 2 * BINS
HALF = BINS - 128
PARTS = WIDTH // 128
GROUP = 8
RUN = 40
MESH = pl.DeviceIdType.MESH


def bin_order():
    bins = np.concatenate([np.arange(BINS), np.arange(128, BINS), np.arange(128)])
    imag = np.arange(WIDTH) >= BINS
    return bins, imag


def angle(product):
    return np.float32(2.0 * math.pi / SAMPLES) * (product % SAMPLES).astype(np.float32)


def forward_table():
    bins, imag = bin_order()
    angles = angle(np.arange(SAMPLES)[:, None] * (FIRST_BIN + bins)[None, :])
    return jnp.asarray(np.where(imag[None, :], -np.sin(angles), np.cos(angles)).astype(np.float32)).astype(jnp.bfloat16)


def lag_tables():
    bins, imag = bin_order()
    delays = LAG_STEP * (np.arange(LAGS) - LAGS // 2)
    angles = angle(delays[:, None] * (FIRST_BIN + bins[:256])[None, :])
    straight = np.cos(angles).astype(np.float32)
    crossed = np.where(imag[None, :256], -np.sin(angles), np.sin(angles)).astype(np.float32)
    tables = np.stack([straight[:, :128], straight[:, 128:], crossed[:, :128], crossed[:, 128:]])
    return jnp.asarray(tables).astype(jnp.bfloat16)


def tile_plan(segments, local):
    lanes = segments * local
    width = 128 if lanes % 128 == 0 else lanes
    tiles = lanes // width
    parts = [(s, t) for s in range(segments) for t in range(PARTS)]
    pieces, stages, done, used = [], [], 0, 0
    for j in range(tiles):
        row = []
        for s in range(segments):
            lo, hi = max(s * local, j * width), min((s + 1) * local, (j + 1) * width)
            if lo < hi:
                row.append((s, lo - j * width, hi - j * width, lo - s * local))
        pieces.append(row)
        whole = (j + 1) * width // local
        if whole > done and j >= tiles - 2:
            ready = whole * PARTS
            ready -= ready % 2 if j < tiles - 1 else 0
            stages.append((j, list(range(done, whole)), parts[used:ready]))
            done, used = whole, ready
    return width, pieces, stages


def turned_pair(rows, mid, lag, parts, base, first):
    halves = []
    for k in range(2):
        i = first + k
        columns = []
        for s, t in parts:
            if t == 1:
                x, y, c = rows[s, 1, pl.ds(base, GROUP), :], mid[s, pl.ds(base, GROUP), :], 1
            else:
                x, y, c = rows[s, t, pl.ds(base, GROUP), :], rows[s, 2 - t, pl.ds(base, GROUP), :], 0
            x, y = (jnp.broadcast_to(v[i:i + 1], (16, 128)).astype(jnp.bfloat16) for v in (x, y))
            column = []
            for m in range(0, LAGS, 16):
                straight, crossed = x * lag[c, m:m + 16], y * lag[c + 2, m:m + 16]
                column.append(straight - crossed if t == 2 else straight + crossed)
            columns.append(jnp.concatenate(column, axis=0))
        halves.append(jnp.concatenate(columns, axis=1))
    return jnp.concatenate(halves, axis=0)


def turn_rows(rows, mid, s, value):
    for t in range(PARTS):
        rows[s, t] = value[:, t * 128:(t + 1) * 128]
    mid[s] = pltpu.roll(value[:, 128:256], HALF, 1)


def lag_dot(right, turned, parts):
    left = jnp.concatenate([right[t] for t in range(parts)], axis=1)
    return lax.dot_general(left, turned, (((1,), (1,)), ((), ())), preferred_element_type=jnp.float32)


def slot_scale(partner, counts, slot):
    live = (partner[0, slot] >= 0).astype(jnp.float32)
    count = jnp.full((8, LAGS), counts[0, slot].astype(jnp.float32), jnp.float32)
    return (lax.rsqrt(count) * (live * (1.0 / math.sqrt(BINS))))[0:1]


def masked(source, s, t, counts, slot):
    return (source[s, t].astype(jnp.float32) * (s < counts[0, slot]).astype(jnp.float32)).astype(jnp.bfloat16)


def exchange_kernel(n, width, pieces, stages, raw, table_hbm, lag_hbm, counts_hbm, own, near, far, acc,
                    raw_v, table, lag, counts, turned, landed, spec, right, rows, mid, load_sem, send_sem, recv_sem, pass_send, pass_recv):
    me = lax.axis_index("row")
    segments, _, block, _ = own.shape
    tiles = len(pieces)
    channels = turned.shape[1]
    barrier = pltpu.get_barrier_semaphore()

    def ahead(k):
        return lax.rem(me + k, n)

    @pl.loop(1, n)
    def _(k):
        pl.semaphore_signal(barrier, inc=1, device_id={"row": ahead(k)}, device_id_type=MESH)

    loads = [pltpu.make_async_copy(raw.at[j], raw_v.at[j], load_sem.at[j]) for j in range(tiles)]
    more = [pltpu.make_async_copy(source, place, load_sem.at[tiles + i]) for i, (source, place) in enumerate(
        ((counts_hbm, counts), (table_hbm, table), (lag_hbm, lag)))]
    for copy in loads + more:
        copy.start()

    def tile_copy(j, k):
        target = ahead(k)
        return pltpu.make_async_remote_copy(
            src_ref=turned.at[j, pl.ds(pl.multiple_of(target * block, 16), block)],
            dst_ref=landed.at[j, me],
            send_sem=send_sem.at[j, k],
            recv_sem=recv_sem.at[j, k],
            device_id={"row": target},
            device_id_type=MESH,
        )

    def send(j, lo, hi):
        @pl.loop(lo, hi)
        def _(k):
            tile_copy(j, k).start()

    half = n // 2

    def send_next(j):
        if tiles > 2 and j < 2:
            for i in range(2, tiles):
                send(i, *((1, half), (half, n))[j])

    for j in range(tiles):
        loads[j].wait()

        @pl.loop(0, channels // 128)
        def _(i):
            part = pl.ds(pl.multiple_of(i * 128, 128), 128)
            turned[j, part, :] = raw_v[j, :, part].T

        if j == 0:
            pl.semaphore_wait(barrier, n - 1)
        send(j, 1, n)

    for copy in more:
        copy.wait()

    def transform(j, source, x, fresh):
        for s, lo, hi, t in pieces[j]:
            part = jnp.dot(x[:, lo:hi], table[source, t:t + hi - lo], preferred_element_type=jnp.float32)
            spec[s] = part if fresh and t == 0 else spec[s] + part

    def spectra_first(j):
        transform(j, me, turned[j, pl.ds(pl.multiple_of(me * block, 16), block), :], True)
        spectra_part(j, 1, half)

    def spectra_part(j, lo, hi):
        @pl.loop(lo, hi)
        def _(k):
            tile_copy(j, k).wait_recv()
            source = lax.rem(me + n - k, n)
            transform(j, source, landed[j, source], False)

    def whiten(segs):
        for s in segs:
            value = spec[s]
            energy = 2.0 * jnp.mean(value * value, axis=-1, keepdims=True)
            white = (value * lax.rsqrt(energy + 1e-06)).astype(jnp.bfloat16)
            for t in range(PARTS):
                own[s, t] = white[:, t * 128:(t + 1) * 128]
            turn_rows(rows, mid, s, white.astype(jnp.float32))

    odd = lax.rem(me, 2) == 1
    senders = (me >= 1, jnp.logical_and(odd, me >= 2), jnp.logical_and(odd, me + 1 < n))

    def pass_copy(stage, segs, kind):
        part = pl.ds(segs[0], len(segs))
        source, place, back = ((own, near, 1), (own, far, 2), (near, far, 1))[kind]
        return pltpu.make_async_remote_copy(
            src_ref=source.at[part], dst_ref=place.at[part], send_sem=pass_send.at[stage, kind],
            recv_sem=pass_recv.at[stage, min(kind, 1)], device_id={"row": ahead(n - back)}, device_id_type=MESH,
        )

    def pass_start(stage, segs):
        for kind in range(2):
            @pl.when(senders[kind])
            def _():
                pass_copy(stage, segs, kind).start()

    def pass_near(stage, segs):
        @pl.when(me + 1 < n)
        def _():
            pass_copy(stage, segs, 0).wait_recv()

        @pl.when(senders[2])
        def _():
            pass_copy(stage, segs, 2).start()

    def pass_far(stage, segs):
        @pl.when(me + 2 < n)
        def _():
            pass_copy(stage, segs, 1).wait_recv()

    def pass_sent(stage, segs):
        for kind, sends in enumerate(senders):
            @pl.when(sends)
            def _():
                pass_copy(stage, segs, kind).wait_send()

    for i, place in enumerate((near, far)):
        @pl.when(me + i + 1 >= n)
        def _():
            place[...] = jnp.zeros_like(place)


    def take_rows(parts):
        for slot, source in enumerate((own, near, far)):
            for at, (s, t) in enumerate(parts):
                right[at, slot * block:(slot + 1) * block] = masked(source, s, t, counts, slot)

    def correlate_rows(parts, total, lo, hi):
        @pl.loop(0, (hi - lo) // RUN)
        def _(g):
            base = pl.multiple_of(lo + g * RUN, GROUP)
            for i in range(0, RUN, 2):
                result = lag_dot(right, turned_pair(rows, mid, lag, parts, base + i // GROUP * GROUP, i % GROUP), len(parts))
                for k in range(2):
                    a = base + i + k
                    for slot in range(SLOTS):
                        part = result[slot * block:(slot + 1) * block, k * LAGS:(k + 1) * LAGS]
                        acc[slot, a] = acc[slot, a] + part if total else part

    last = len(stages) - 1
    middle = block // 2 // RUN * RUN
    if not last:
        acc[...] = jnp.zeros_like(acc)

    def spectra(j):
        spectra_first(j)
        spectra_part(j, half, n)

    def arrive(stage):
        segs = stages[stage][1]
        pass_near(stage, segs)
        pass_far(stage, segs)

    for stage, (j, segs, parts) in enumerate(stages):
        for i in range(stages[stage - 1][0] + 1 if stage else 0, j + 1):
            spectra(i)
        whiten(segs)
        pass_start(stage, segs)
        if 0 < stage:
            arrive(stage - 1)
            take_rows(stages[stage - 1][2])
            correlate_rows(stages[stage - 1][2], stage > 1, 0, middle)
            if stage == last:
                pass_near(stage, segs)
            correlate_rows(stages[stage - 1][2], stage > 1, middle, block)
    if not last:
        pass_near(last, stages[last][1])
    for j in range(tiles):
        @pl.loop(1, n)
        def _(k):
            tile_copy(j, k).wait_send()
    pass_far(last, stages[last][1])
    for stage, (_, segs, _) in enumerate(stages):
        pass_sent(stage, segs)


def exchange(raw_samples, counts, width, pieces, stages):
    n = lax.axis_size("row")
    segments, local, channels = raw_samples.shape
    block = channels // n
    tiles = len(pieces)
    parts = max(len(parts) for _, _, parts in stages)
    white = jax.ShapeDtypeStruct((segments, PARTS, block, 128), jnp.bfloat16)
    vmem = pl.BlockSpec(memory_space=pltpu.VMEM)
    hbm = pl.BlockSpec(memory_space=pltpu.HBM)
    inputs = (raw_samples.reshape(tiles, width, channels), forward_table().reshape(n, local, WIDTH), lag_tables(), counts)
    return pl.pallas_call(
        functools.partial(exchange_kernel, n, width, pieces, stages),
        out_shape=(white,) * 3 + (jax.ShapeDtypeStruct((SLOTS, block, block, LAGS), jnp.float32),),
        in_specs=[hbm] * 4,
        out_specs=(vmem,) * 4,
        scratch_shapes=[
            pltpu.VMEM((tiles, width, channels), jnp.bfloat16),
            pltpu.VMEM((n, local, WIDTH), jnp.bfloat16),
            pltpu.VMEM((4, LAGS, 128), jnp.bfloat16),
            pltpu.SMEM((1, SLOTS), jnp.int32),
            pltpu.VMEM((tiles, channels, width), jnp.bfloat16),
            pltpu.VMEM((tiles, n, block, width), jnp.bfloat16),
            pltpu.VMEM((segments, block, WIDTH), jnp.float32),
            pltpu.VMEM((parts, SLOTS * block, 128), jnp.bfloat16),
            pltpu.VMEM((segments, PARTS, block, 128), jnp.float32),
            pltpu.VMEM((segments, block, 128), jnp.float32),
            pltpu.SemaphoreType.DMA((tiles + 3,)),
            pltpu.SemaphoreType.DMA((tiles, n)),
            pltpu.SemaphoreType.DMA((tiles, n)),
            pltpu.SemaphoreType.DMA((len(stages), 3)),
            pltpu.SemaphoreType.DMA((len(stages), 2)),
        ],
        compiler_params=pltpu.CompilerParams(collective_id=0, has_side_effects=True, vmem_limit_bytes=20_000_000),
        cost_estimate=pl.CostEstimate(flops=20_000_000_000, bytes_accessed=4_000_000, transcendentals=0),
        name="exchange",
    )(*(pltpu.with_memory_space_constraint(x, pltpu.HBM) for x in inputs))


def correlate_kernel(parts, partner, counts, own, near, far, acc, lag_in, out, staged, right, rows, mid, lag, out_sem):
    block = own.shape[2]
    for slot, source in enumerate((own, near, far)):
        for at, (s, t) in enumerate(parts):
            right[at, slot * block:(slot + 1) * block] = masked(source, s, t, counts, slot)
    for s in sorted({s for s, _ in parts}):
        turn_rows(rows, mid, s, jnp.concatenate([own[s, t].astype(jnp.float32) for t in range(PARTS)], axis=1))
    lag[...] = lag_in[...]
    scales = [slot_scale(partner, counts, slot) for slot in range(SLOTS)]

    def write(g):
        here = pl.ds(g * GROUP, GROUP)
        return pltpu.make_async_copy(staged.at[:, here], out.at[0, :, here], out_sem.at[g])

    for a in range(0, block, 2):
        result = lag_dot(right, turned_pair(rows, mid, lag, parts, a // GROUP * GROUP, a % GROUP), len(parts))
        for k in range(2):
            for slot in range(SLOTS):
                part = result[slot * block:(slot + 1) * block, k * LAGS:(k + 1) * LAGS]
                part = (acc[slot, a + k] + part) * scales[slot]
                if slot == 0:
                    part = jnp.where(lax.broadcasted_iota(jnp.int32, part.shape, 0) > a + k, part, 0.0)
                staged[slot, a + k] = part.astype(jnp.bfloat16)
        if (a + 2) % GROUP == 0:
            write(a // GROUP).start()
    for g in range(block // GROUP):
        write(g).wait()


def correlate(parts, partner, counts, own, near, far, acc):
    segments, _, block, _ = own.shape
    vmem = pl.BlockSpec(memory_space=pltpu.VMEM)
    return pl.pallas_call(
        functools.partial(correlate_kernel, parts),
        in_specs=[pl.BlockSpec(memory_space=pltpu.SMEM)] * 2 + [vmem] * 5,
        out_specs=pl.BlockSpec(memory_space=pltpu.HBM),
        scratch_shapes=[
            pltpu.VMEM((SLOTS, block, block, LAGS), jnp.bfloat16),
            pltpu.VMEM((len(parts), SLOTS * block, 128), jnp.bfloat16),
            pltpu.VMEM((segments, PARTS, block, 128), jnp.float32),
            pltpu.VMEM((segments, block, 128), jnp.float32),
            pltpu.VMEM((4, LAGS, 128), jnp.bfloat16),
            pltpu.SemaphoreType.DMA((block // GROUP,)),
        ],
        out_shape=jax.ShapeDtypeStruct((1, SLOTS, block, block, LAGS), jnp.bfloat16),
        cost_estimate=pl.CostEstimate(
            flops=6 * block * block * LAGS * len(parts) * 128, bytes_accessed=6_000_000, transcendentals=0),
        compiler_params=pltpu.CompilerParams(vmem_limit_bytes=15 * 2**20),
        name="correlate",
    )(partner, counts, own, near, far, acc, lag_tables())


def on_device(raw_samples, partner, counts):
    width, pieces, stages = tile_plan(raw_samples.shape[0], raw_samples.shape[1])
    own, near, far, acc = exchange(raw_samples, counts, width, pieces, stages)
    return correlate(stages[-1][2], partner, counts, own, near, far, acc)


def solution(mesh):
    return jax.shard_map(
        on_device,
        mesh=mesh,
        in_specs=(P("groups", "row", None), P(("groups", "row"), None), P(("groups", "row"), None)),
        out_specs=P(("groups", "row"), None, None, None, None),
        check_vma=False,
    )
```

```python
import functools
import math

import jax
import jax.numpy as jnp
import numpy as np
from jax import lax
from jax.experimental import pallas as pl
from jax.experimental.pallas import tpu as pltpu
from jax.sharding import PartitionSpec as P

SAMPLES = 1536
BINS = 192
FIRST_BIN = 5
LAGS = 128
LAG_STEP = 4
SLOTS = 3
WIDTH = 2 * BINS
HALF = BINS - 128
PARTS = WIDTH // 128
GROUP = 8
MESH = pl.DeviceIdType.MESH


def bin_order():
    bins = np.concatenate([np.arange(BINS), np.arange(128, BINS), np.arange(128)])
    imag = np.arange(WIDTH) >= BINS
    return bins, imag


def angle(product):
    return np.float32(2.0 * math.pi / SAMPLES) * (product % SAMPLES).astype(np.float32)


def forward_table():
    bins, imag = bin_order()
    angles = angle(np.arange(SAMPLES)[:, None] * (FIRST_BIN + bins)[None, :])
    return jnp.asarray(np.where(imag[None, :], -np.sin(angles), np.cos(angles)).astype(np.float32)).astype(jnp.bfloat16)


def lag_tables():
    bins, imag = bin_order()
    delays = LAG_STEP * (np.arange(LAGS) - LAGS // 2)
    angles = angle(delays[:, None] * (FIRST_BIN + bins[:256])[None, :])
    straight = np.cos(angles).astype(np.float32)
    crossed = np.where(imag[None, :256], -np.sin(angles), np.sin(angles)).astype(np.float32)
    tables = np.stack([straight[:, :128], straight[:, 128:], crossed[:, :128], crossed[:, 128:]])
    return jnp.asarray(tables).astype(jnp.bfloat16)


def tile_plan(segments, local):
    lanes = segments * local
    width = 128 if lanes % 128 == 0 else lanes
    tiles = lanes // width
    parts = [(s, t) for s in range(segments) for t in range(PARTS)]
    pieces, stages, done, used = [], [], 0, 0
    for j in range(tiles):
        row = []
        for s in range(segments):
            lo, hi = max(s * local, j * width), min((s + 1) * local, (j + 1) * width)
            if lo < hi:
                row.append((s, lo - j * width, hi - j * width, lo - s * local))
        pieces.append(row)
        whole = (j + 1) * width // local
        if whole > done and j >= tiles - 2:
            ready = whole * PARTS
            ready -= ready % 2 if j < tiles - 1 else 0
            stages.append((j, list(range(done, whole)), parts[used:ready]))
            done, used = whole, ready
    return width, pieces, stages


def turned_pair(rows, mid, lag, parts, base, first):
    halves = []
    for k in range(2):
        i = first + k
        columns = []
        for s, t in parts:
            if t == 1:
                x, y, c = rows[s, 1, pl.ds(base, GROUP), :], mid[s, pl.ds(base, GROUP), :], 1
            else:
                x, y, c = rows[s, t, pl.ds(base, GROUP), :], rows[s, 2 - t, pl.ds(base, GROUP), :], 0
            x, y = (jnp.broadcast_to(v[i:i + 1], (16, 128)).astype(jnp.bfloat16) for v in (x, y))
            column = []
            for m in range(0, LAGS, 16):
                straight, crossed = x * lag[c, m:m + 16], y * lag[c + 2, m:m + 16]
                column.append(straight - crossed if t == 2 else straight + crossed)
            columns.append(jnp.concatenate(column, axis=0))
        halves.append(jnp.concatenate(columns, axis=1))
    return jnp.concatenate(halves, axis=0)


def turn_rows(rows, mid, s, value):
    for t in range(PARTS):
        rows[s, t] = value[:, t * 128:(t + 1) * 128]
    mid[s] = pltpu.roll(value[:, 128:256], HALF, 1)


def lag_dot(right, turned, parts):
    left = jnp.concatenate([right[t] for t in range(parts)], axis=1)
    return lax.dot_general(left, turned, (((1,), (1,)), ((), ())), preferred_element_type=jnp.float32)


def slot_scale(partner, counts, slot):
    live = (partner[0, slot] >= 0).astype(jnp.float32)
    count = jnp.full((8, LAGS), counts[0, slot].astype(jnp.float32), jnp.float32)
    return (lax.rsqrt(count) * (live * (1.0 / math.sqrt(BINS))))[0:1]


def masked(source, s, t, counts, slot):
    return (source[s, t].astype(jnp.float32) * (s < counts[0, slot]).astype(jnp.float32)).astype(jnp.bfloat16)


def exchange_kernel(n, width, pieces, stages, raw, table_hbm, lag_hbm, counts_hbm, own, near, far, acc,
                    raw_v, table, lag, counts, turned, landed, spec, right, rows, mid, load_sem, send_sem, recv_sem, pass_send, pass_recv):
    me = lax.axis_index("row")
    segments, _, block, _ = own.shape
    tiles = len(pieces)
    channels = turned.shape[1]
    barrier = pltpu.get_barrier_semaphore()

    def ahead(k):
        return lax.rem(me + k, n)

    @pl.loop(1, n)
    def _(k):
        pl.semaphore_signal(barrier, inc=1, device_id={"row": ahead(k)}, device_id_type=MESH)

    loads = [pltpu.make_async_copy(raw.at[j], raw_v.at[j], load_sem.at[j]) for j in range(tiles)]
    more = [pltpu.make_async_copy(source, place, load_sem.at[tiles + i]) for i, (source, place) in enumerate(
        ((counts_hbm, counts), (table_hbm, table), (lag_hbm, lag)))]
    for copy in loads + more:
        copy.start()

    def tile_copy(j, k):
        target = ahead(k)
        return pltpu.make_async_remote_copy(
            src_ref=turned.at[j, pl.ds(pl.multiple_of(target * block, 16), block)],
            dst_ref=landed.at[j, me],
            send_sem=send_sem.at[j, k],
            recv_sem=recv_sem.at[j, k],
            device_id={"row": target},
            device_id_type=MESH,
        )

    def send(j, lo, hi):
        @pl.loop(lo, hi)
        def _(k):
            tile_copy(j, k).start()

    half = n // 2

    def send_next(j):
        if tiles > 2 and j < 2:
            for i in range(2, tiles):
                send(i, *((1, half), (half, n))[j])

    for j in range(tiles):
        loads[j].wait()

        @pl.loop(0, channels // 128)
        def _(i):
            part = pl.ds(pl.multiple_of(i * 128, 128), 128)
            turned[j, part, :] = raw_v[j, :, part].T

        if j == 0:
            pl.semaphore_wait(barrier, n - 1)
        send(j, 1, n)

    for copy in more:
        copy.wait()

    def transform(j, source, x, fresh):
        for s, lo, hi, t in pieces[j]:
            part = jnp.dot(x[:, lo:hi], table[source, t:t + hi - lo], preferred_element_type=jnp.float32)
            spec[s] = part if fresh and t == 0 else spec[s] + part

    def spectra_first(j):
        transform(j, me, turned[j, pl.ds(pl.multiple_of(me * block, 16), block), :], True)
        spectra_part(j, 1, half)

    def spectra_part(j, lo, hi):
        @pl.loop(lo, hi)
        def _(k):
            tile_copy(j, k).wait_recv()
            source = lax.rem(me + n - k, n)
            transform(j, source, landed[j, source], False)

    def whiten(segs):
        for s in segs:
            value = spec[s]
            energy = 2.0 * jnp.mean(value * value, axis=-1, keepdims=True)
            white = (value * lax.rsqrt(energy + 1e-06)).astype(jnp.bfloat16)
            for t in range(PARTS):
                own[s, t] = white[:, t * 128:(t + 1) * 128]
            turn_rows(rows, mid, s, white.astype(jnp.float32))

    odd = lax.rem(me, 2) == 1
    senders = (me >= 1, jnp.logical_and(odd, me >= 2), jnp.logical_and(odd, me + 1 < n))

    def pass_copy(stage, segs, kind):
        part = pl.ds(segs[0], len(segs))
        source, place, back = ((own, near, 1), (own, far, 2), (near, far, 1))[kind]
        return pltpu.make_async_remote_copy(
            src_ref=source.at[part], dst_ref=place.at[part], send_sem=pass_send.at[stage, kind],
            recv_sem=pass_recv.at[stage, min(kind, 1)], device_id={"row": ahead(n - back)}, device_id_type=MESH,
        )

    def pass_start(stage, segs):
        for kind in range(2):
            @pl.when(senders[kind])
            def _():
                pass_copy(stage, segs, kind).start()

    def pass_near(stage, segs):
        @pl.when(me + 1 < n)
        def _():
            pass_copy(stage, segs, 0).wait_recv()

        @pl.when(senders[2])
        def _():
            pass_copy(stage, segs, 2).start()

    def pass_far(stage, segs):
        @pl.when(me + 2 < n)
        def _():
            pass_copy(stage, segs, 1).wait_recv()

    def pass_sent(stage, segs):
        for kind, sends in enumerate(senders):
            @pl.when(sends)
            def _():
                pass_copy(stage, segs, kind).wait_send()

    for i, place in enumerate((near, far)):
        @pl.when(me + i + 1 >= n)
        def _():
            place[...] = jnp.zeros_like(place)


    def take_rows(parts):
        for slot, source in enumerate((own, near, far)):
            for at, (s, t) in enumerate(parts):
                right[at, slot * block:(slot + 1) * block] = masked(source, s, t, counts, slot)

    def correlate_rows(parts, total, lo, hi):
        for a in range(lo, hi, 2):
            result = lag_dot(right, turned_pair(rows, mid, lag, parts, a // GROUP * GROUP, a % GROUP), len(parts))
            for k in range(2):
                for slot in range(SLOTS):
                    part = result[slot * block:(slot + 1) * block, k * LAGS:(k + 1) * LAGS]
                    acc[slot, a + k] = acc[slot, a + k] + part if total else part

    last = len(stages) - 1
    middle = block * 8 // 10 // GROUP * GROUP
    if not last:
        acc[...] = jnp.zeros_like(acc)

    def spectra(j):
        spectra_first(j)
        spectra_part(j, half, n)

    def arrive(stage):
        segs = stages[stage][1]
        pass_near(stage, segs)
        pass_far(stage, segs)

    for stage, (j, segs, parts) in enumerate(stages):
        for i in range(stages[stage - 1][0] + 1 if stage else 0, j + 1):
            spectra(i)
        whiten(segs)
        pass_start(stage, segs)
        if 0 < stage:
            arrive(stage - 1)
            take_rows(stages[stage - 1][2])
            correlate_rows(stages[stage - 1][2], stage > 1, 0, middle)
            if stage == last:
                pass_near(stage, segs)
            correlate_rows(stages[stage - 1][2], stage > 1, middle, block)
    if not last:
        pass_near(last, stages[last][1])
    for j in range(tiles):
        @pl.loop(1, n)
        def _(k):
            tile_copy(j, k).wait_send()
    pass_far(last, stages[last][1])
    for stage, (_, segs, _) in enumerate(stages):
        pass_sent(stage, segs)


def exchange(raw_samples, counts, width, pieces, stages):
    n = lax.axis_size("row")
    segments, local, channels = raw_samples.shape
    block = channels // n
    tiles = len(pieces)
    parts = max(len(parts) for _, _, parts in stages)
    white = jax.ShapeDtypeStruct((segments, PARTS, block, 128), jnp.bfloat16)
    vmem = pl.BlockSpec(memory_space=pltpu.VMEM)
    hbm = pl.BlockSpec(memory_space=pltpu.HBM)
    inputs = (raw_samples.reshape(tiles, width, channels), forward_table().reshape(n, local, WIDTH), lag_tables(), counts)
    return pl.pallas_call(
        functools.partial(exchange_kernel, n, width, pieces, stages),
        out_shape=(white,) * 3 + (jax.ShapeDtypeStruct((SLOTS, block, block, LAGS), jnp.float32),),
        in_specs=[hbm] * 4,
        out_specs=(vmem,) * 4,
        scratch_shapes=[
            pltpu.VMEM((tiles, width, channels), jnp.bfloat16),
            pltpu.VMEM((n, local, WIDTH), jnp.bfloat16),
            pltpu.VMEM((4, LAGS, 128), jnp.bfloat16),
            pltpu.SMEM((1, SLOTS), jnp.int32),
            pltpu.VMEM((tiles, channels, width), jnp.bfloat16),
            pltpu.VMEM((tiles, n, block, width), jnp.bfloat16),
            pltpu.VMEM((segments, block, WIDTH), jnp.float32),
            pltpu.VMEM((parts, SLOTS * block, 128), jnp.bfloat16),
            pltpu.VMEM((segments, PARTS, block, 128), jnp.float32),
            pltpu.VMEM((segments, block, 128), jnp.float32),
            pltpu.SemaphoreType.DMA((tiles + 3,)),
            pltpu.SemaphoreType.DMA((tiles, n)),
            pltpu.SemaphoreType.DMA((tiles, n)),
            pltpu.SemaphoreType.DMA((len(stages), 3)),
            pltpu.SemaphoreType.DMA((len(stages), 2)),
        ],
        compiler_params=pltpu.CompilerParams(collective_id=0, has_side_effects=True, vmem_limit_bytes=20_000_000),
        cost_estimate=pl.CostEstimate(flops=20_000_000_000, bytes_accessed=4_000_000, transcendentals=0),
        name="exchange",
    )(*(pltpu.with_memory_space_constraint(x, pltpu.HBM) for x in inputs))


def correlate_kernel(parts, partner, counts, own, near, far, acc, lag_in, out, staged, right, rows, mid, lag, out_sem):
    block = own.shape[2]
    for slot, source in enumerate((own, near, far)):
        for at, (s, t) in enumerate(parts):
            right[at, slot * block:(slot + 1) * block] = masked(source, s, t, counts, slot)
    for s in sorted({s for s, _ in parts}):
        turn_rows(rows, mid, s, jnp.concatenate([own[s, t].astype(jnp.float32) for t in range(PARTS)], axis=1))
    lag[...] = lag_in[...]
    scales = [slot_scale(partner, counts, slot) for slot in range(SLOTS)]

    def write(g):
        here = pl.ds(g * GROUP, GROUP)
        return pltpu.make_async_copy(staged.at[:, here], out.at[0, :, here], out_sem.at[g])

    for a in range(0, block, 2):
        result = lag_dot(right, turned_pair(rows, mid, lag, parts, a // GROUP * GROUP, a % GROUP), len(parts))
        for k in range(2):
            for slot in range(SLOTS):
                part = result[slot * block:(slot + 1) * block, k * LAGS:(k + 1) * LAGS]
                part = (acc[slot, a + k] + part) * scales[slot]
                if slot == 0:
                    part = jnp.where(lax.broadcasted_iota(jnp.int32, part.shape, 0) > a + k, part, 0.0)
                staged[slot, a + k] = part.astype(jnp.bfloat16)
        if (a + 2) % GROUP == 0:
            write(a // GROUP).start()
    for g in range(block // GROUP):
        write(g).wait()


def correlate(parts, partner, counts, own, near, far, acc):
    segments, _, block, _ = own.shape
    vmem = pl.BlockSpec(memory_space=pltpu.VMEM)
    return pl.pallas_call(
        functools.partial(correlate_kernel, parts),
        in_specs=[pl.BlockSpec(memory_space=pltpu.SMEM)] * 2 + [vmem] * 5,
        out_specs=pl.BlockSpec(memory_space=pltpu.HBM),
        scratch_shapes=[
            pltpu.VMEM((SLOTS, block, block, LAGS), jnp.bfloat16),
            pltpu.VMEM((len(parts), SLOTS * block, 128), jnp.bfloat16),
            pltpu.VMEM((segments, PARTS, block, 128), jnp.float32),
            pltpu.VMEM((segments, block, 128), jnp.float32),
            pltpu.VMEM((4, LAGS, 128), jnp.bfloat16),
            pltpu.SemaphoreType.DMA((block // GROUP,)),
        ],
        out_shape=jax.ShapeDtypeStruct((1, SLOTS, block, block, LAGS), jnp.bfloat16),
        cost_estimate=pl.CostEstimate(
            flops=6 * block * block * LAGS * len(parts) * 128, bytes_accessed=6_000_000, transcendentals=0),
        compiler_params=pltpu.CompilerParams(vmem_limit_bytes=15 * 2**20),
        name="correlate",
    )(partner, counts, own, near, far, acc, lag_tables())


def on_device(raw_samples, partner, counts):
    width, pieces, stages = tile_plan(raw_samples.shape[0], raw_samples.shape[1])
    own, near, far, acc = exchange(raw_samples, counts, width, pieces, stages)
    return correlate(stages[-1][2], partner, counts, own, near, far, acc)


def solution(mesh):
    return jax.shard_map(
        on_device,
        mesh=mesh,
        in_specs=(P("groups", "row", None), P(("groups", "row"), None), P(("groups", "row"), None)),
        out_specs=P(("groups", "row"), None, None, None, None),
        check_vma=False,
    )
```

```python
import functools
import math

import jax
import jax.numpy as jnp
import numpy as np
from jax import lax
from jax.experimental import pallas as pl
from jax.experimental.pallas import tpu as pltpu
from jax.sharding import PartitionSpec as P

SAMPLES = 1536
BINS = 192
FIRST_BIN = 5
LAGS = 128
LAG_STEP = 4
SLOTS = 3
WIDTH = 2 * BINS
HALF = BINS - 128
PARTS = WIDTH // 128
GROUP = 8
RUN = 80
MESH = pl.DeviceIdType.MESH


def bin_order():
    bins = np.concatenate([np.arange(BINS), np.arange(128, BINS), np.arange(128)])
    imag = np.arange(WIDTH) >= BINS
    return bins, imag


def angle(product):
    return np.float32(2.0 * math.pi / SAMPLES) * (product % SAMPLES).astype(np.float32)


def forward_table():
    bins, imag = bin_order()
    angles = angle(np.arange(SAMPLES)[:, None] * (FIRST_BIN + bins)[None, :])
    return jnp.asarray(np.where(imag[None, :], -np.sin(angles), np.cos(angles)).astype(np.float32)).astype(jnp.bfloat16)


def lag_tables():
    bins, imag = bin_order()
    delays = LAG_STEP * (np.arange(LAGS) - LAGS // 2)
    angles = angle(delays[:, None] * (FIRST_BIN + bins[:256])[None, :])
    straight = np.cos(angles).astype(np.float32)
    crossed = np.where(imag[None, :256], -np.sin(angles), np.sin(angles)).astype(np.float32)
    tables = np.stack([straight[:, :128], straight[:, 128:], crossed[:, :128], crossed[:, 128:]])
    return jnp.asarray(tables).astype(jnp.bfloat16)


def tile_plan(segments, local):
    lanes = segments * local
    width = 128 if lanes % 128 == 0 else lanes
    tiles = lanes // width
    parts = [(s, t) for s in range(segments) for t in range(PARTS)]
    pieces, stages, done, used = [], [], 0, 0
    for j in range(tiles):
        row = []
        for s in range(segments):
            lo, hi = max(s * local, j * width), min((s + 1) * local, (j + 1) * width)
            if lo < hi:
                row.append((s, lo - j * width, hi - j * width, lo - s * local))
        pieces.append(row)
        whole = (j + 1) * width // local
        if whole > done and j >= tiles - 2:
            ready = whole * PARTS
            ready -= ready % 2 if j < tiles - 1 else 0
            stages.append((j, list(range(done, whole)), parts[used:ready]))
            done, used = whole, ready
    return width, pieces, stages


def turned_pair(rows, mid, lag, parts, base, first):
    halves = []
    for k in range(2):
        i = first + k
        columns = []
        for s, t in parts:
            if t == 1:
                x, y, c = rows[s, 1, pl.ds(base, GROUP), :], mid[s, pl.ds(base, GROUP), :], 1
            else:
                x, y, c = rows[s, t, pl.ds(base, GROUP), :], rows[s, 2 - t, pl.ds(base, GROUP), :], 0
            x, y = (jnp.broadcast_to(v[i:i + 1], (16, 128)).astype(jnp.bfloat16) for v in (x, y))
            column = []
            for m in range(0, LAGS, 16):
                straight, crossed = x * lag[c, m:m + 16], y * lag[c + 2, m:m + 16]
                column.append(straight - crossed if t == 2 else straight + crossed)
            columns.append(jnp.concatenate(column, axis=0))
        halves.append(jnp.concatenate(columns, axis=1))
    return jnp.concatenate(halves, axis=0)


def turn_rows(rows, mid, s, value):
    for t in range(PARTS):
        rows[s, t] = value[:, t * 128:(t + 1) * 128]
    mid[s] = pltpu.roll(value[:, 128:256], HALF, 1)


def lag_dot(right, turned, parts):
    left = jnp.concatenate([right[t] for t in range(parts)], axis=1)
    return lax.dot_general(left, turned, (((1,), (1,)), ((), ())), preferred_element_type=jnp.float32)


def slot_scale(partner, counts, slot):
    live = (partner[0, slot] >= 0).astype(jnp.float32)
    count = jnp.full((8, LAGS), counts[0, slot].astype(jnp.float32), jnp.float32)
    return (lax.rsqrt(count) * (live * (1.0 / math.sqrt(BINS))))[0:1]


def masked(source, s, t, counts, slot):
    return (source[s, t].astype(jnp.float32) * (s < counts[0, slot]).astype(jnp.float32)).astype(jnp.bfloat16)


def exchange_kernel(n, width, pieces, stages, raw, table_hbm, lag_hbm, counts_hbm, own, near, far, acc,
                    raw_v, table, lag, counts, turned, landed, spec, right, rows, mid, load_sem, send_sem, recv_sem, pass_send, pass_recv):
    me = lax.axis_index("row")
    segments, _, block, _ = own.shape
    tiles = len(pieces)
    channels = turned.shape[1]
    barrier = pltpu.get_barrier_semaphore()

    def ahead(k):
        return lax.rem(me + k, n)

    @pl.loop(1, n)
    def _(k):
        pl.semaphore_signal(barrier, inc=1, device_id={"row": ahead(k)}, device_id_type=MESH)

    loads = [pltpu.make_async_copy(raw.at[j], raw_v.at[j], load_sem.at[j]) for j in range(tiles)]
    more = [pltpu.make_async_copy(source, place, load_sem.at[tiles + i]) for i, (source, place) in enumerate(
        ((counts_hbm, counts), (table_hbm, table), (lag_hbm, lag)))]
    for copy in loads + more:
        copy.start()

    def tile_copy(j, k):
        target = ahead(k)
        return pltpu.make_async_remote_copy(
            src_ref=turned.at[j, pl.ds(pl.multiple_of(target * block, 16), block)],
            dst_ref=landed.at[j, me],
            send_sem=send_sem.at[j, k],
            recv_sem=recv_sem.at[j, k],
            device_id={"row": target},
            device_id_type=MESH,
        )

    def send(j, lo, hi):
        @pl.loop(lo, hi)
        def _(k):
            tile_copy(j, k).start()

    half = n // 2

    def send_next(j):
        if tiles > 2 and j < 2:
            for i in range(2, tiles):
                send(i, *((1, half), (half, n))[j])

    for j in range(tiles):
        loads[j].wait()

        @pl.loop(0, channels // 128)
        def _(i):
            part = pl.ds(pl.multiple_of(i * 128, 128), 128)
            turned[j, part, :] = raw_v[j, :, part].T

        if j == 0:
            pl.semaphore_wait(barrier, n - 1)
        send(j, 1, n)

    for copy in more:
        copy.wait()

    def transform(j, source, x, fresh):
        for s, lo, hi, t in pieces[j]:
            part = jnp.dot(x[:, lo:hi], table[source, t:t + hi - lo], preferred_element_type=jnp.float32)
            spec[s] = part if fresh and t == 0 else spec[s] + part

    def spectra_first(j):
        transform(j, me, turned[j, pl.ds(pl.multiple_of(me * block, 16), block), :], True)
        spectra_part(j, 1, half)

    def spectra_part(j, lo, hi):
        @pl.loop(lo, hi)
        def _(k):
            tile_copy(j, k).wait_recv()
            source = lax.rem(me + n - k, n)
            transform(j, source, landed[j, source], False)

    def whiten(segs):
        for s in segs:
            value = spec[s]
            energy = 2.0 * jnp.mean(value * value, axis=-1, keepdims=True)
            white = (value * lax.rsqrt(energy + 1e-06)).astype(jnp.bfloat16)
            for t in range(PARTS):
                own[s, t] = white[:, t * 128:(t + 1) * 128]
            turn_rows(rows, mid, s, white.astype(jnp.float32))

    odd = lax.rem(me, 2) == 1
    senders = (me >= 1, jnp.logical_and(odd, me >= 2), jnp.logical_and(odd, me + 1 < n))

    def pass_copy(stage, segs, kind):
        part = pl.ds(segs[0], len(segs))
        source, place, back = ((own, near, 1), (own, far, 2), (near, far, 1))[kind]
        return pltpu.make_async_remote_copy(
            src_ref=source.at[part], dst_ref=place.at[part], send_sem=pass_send.at[stage, kind],
            recv_sem=pass_recv.at[stage, min(kind, 1)], device_id={"row": ahead(n - back)}, device_id_type=MESH,
        )

    def pass_start(stage, segs):
        for kind in range(2):
            @pl.when(senders[kind])
            def _():
                pass_copy(stage, segs, kind).start()

    def pass_near(stage, segs):
        @pl.when(me + 1 < n)
        def _():
            pass_copy(stage, segs, 0).wait_recv()

        @pl.when(senders[2])
        def _():
            pass_copy(stage, segs, 2).start()

    def pass_far(stage, segs):
        @pl.when(me + 2 < n)
        def _():
            pass_copy(stage, segs, 1).wait_recv()

    def pass_sent(stage, segs):
        for kind, sends in enumerate(senders):
            @pl.when(sends)
            def _():
                pass_copy(stage, segs, kind).wait_send()

    for i, place in enumerate((near, far)):
        @pl.when(me + i + 1 >= n)
        def _():
            place[...] = jnp.zeros_like(place)


    def take_rows(parts):
        for slot, source in enumerate((own, near, far)):
            for at, (s, t) in enumerate(parts):
                right[at, slot * block:(slot + 1) * block] = masked(source, s, t, counts, slot)

    def correlate_rows(parts, total, lo, hi):
        @pl.loop(0, (hi - lo) // RUN)
        def _(g):
            base = pl.multiple_of(lo + g * RUN, GROUP)
            for i in range(0, RUN, 2):
                result = lag_dot(right, turned_pair(rows, mid, lag, parts, base + i // GROUP * GROUP, i % GROUP), len(parts))
                for k in range(2):
                    a = base + i + k
                    for slot in range(SLOTS):
                        part = result[slot * block:(slot + 1) * block, k * LAGS:(k + 1) * LAGS]
                        acc[slot, a] = acc[slot, a] + part if total else part

    last = len(stages) - 1
    middle = block // 2 // RUN * RUN
    if not last:
        acc[...] = jnp.zeros_like(acc)

    def spectra(j):
        spectra_first(j)
        spectra_part(j, half, n)

    def arrive(stage):
        segs = stages[stage][1]
        pass_near(stage, segs)
        pass_far(stage, segs)

    for stage, (j, segs, parts) in enumerate(stages):
        for i in range(stages[stage - 1][0] + 1 if stage else 0, j + 1):
            spectra(i)
        whiten(segs)
        pass_start(stage, segs)
        if 0 < stage:
            arrive(stage - 1)
            take_rows(stages[stage - 1][2])
            correlate_rows(stages[stage - 1][2], stage > 1, 0, block)
            if stage == last:
                pass_near(stage, segs)
    if not last:
        pass_near(last, stages[last][1])
    for j in range(tiles):
        @pl.loop(1, n)
        def _(k):
            tile_copy(j, k).wait_send()
    pass_far(last, stages[last][1])
    for stage, (_, segs, _) in enumerate(stages):
        pass_sent(stage, segs)


def exchange(raw_samples, counts, width, pieces, stages):
    n = lax.axis_size("row")
    segments, local, channels = raw_samples.shape
    block = channels // n
    tiles = len(pieces)
    parts = max(len(parts) for _, _, parts in stages)
    white = jax.ShapeDtypeStruct((segments, PARTS, block, 128), jnp.bfloat16)
    vmem = pl.BlockSpec(memory_space=pltpu.VMEM)
    hbm = pl.BlockSpec(memory_space=pltpu.HBM)
    inputs = (raw_samples.reshape(tiles, width, channels), forward_table().reshape(n, local, WIDTH), lag_tables(), counts)
    return pl.pallas_call(
        functools.partial(exchange_kernel, n, width, pieces, stages),
        out_shape=(white,) * 3 + (jax.ShapeDtypeStruct((SLOTS, block, block, LAGS), jnp.float32),),
        in_specs=[hbm] * 4,
        out_specs=(vmem,) * 4,
        scratch_shapes=[
            pltpu.VMEM((tiles, width, channels), jnp.bfloat16),
            pltpu.VMEM((n, local, WIDTH), jnp.bfloat16),
            pltpu.VMEM((4, LAGS, 128), jnp.bfloat16),
            pltpu.SMEM((1, SLOTS), jnp.int32),
            pltpu.VMEM((tiles, channels, width), jnp.bfloat16),
            pltpu.VMEM((tiles, n, block, width), jnp.bfloat16),
            pltpu.VMEM((segments, block, WIDTH), jnp.float32),
            pltpu.VMEM((parts, SLOTS * block, 128), jnp.bfloat16),
            pltpu.VMEM((segments, PARTS, block, 128), jnp.float32),
            pltpu.VMEM((segments, block, 128), jnp.float32),
            pltpu.SemaphoreType.DMA((tiles + 3,)),
            pltpu.SemaphoreType.DMA((tiles, n)),
            pltpu.SemaphoreType.DMA((tiles, n)),
            pltpu.SemaphoreType.DMA((len(stages), 3)),
            pltpu.SemaphoreType.DMA((len(stages), 2)),
        ],
        compiler_params=pltpu.CompilerParams(collective_id=0, has_side_effects=True, vmem_limit_bytes=20_000_000),
        cost_estimate=pl.CostEstimate(flops=20_000_000_000, bytes_accessed=4_000_000, transcendentals=0),
        name="exchange",
    )(*(pltpu.with_memory_space_constraint(x, pltpu.HBM) for x in inputs))


def correlate_kernel(parts, partner, counts, own, near, far, acc, lag_in, out, staged, right, rows, mid, lag, out_sem):
    block = own.shape[2]
    for slot, source in enumerate((own, near, far)):
        for at, (s, t) in enumerate(parts):
            right[at, slot * block:(slot + 1) * block] = masked(source, s, t, counts, slot)
    for s in sorted({s for s, _ in parts}):
        turn_rows(rows, mid, s, jnp.concatenate([own[s, t].astype(jnp.float32) for t in range(PARTS)], axis=1))
    lag[...] = lag_in[...]
    scales = [slot_scale(partner, counts, slot) for slot in range(SLOTS)]

    def write(g):
        here = pl.ds(g * GROUP, GROUP)
        return pltpu.make_async_copy(staged.at[:, here], out.at[0, :, here], out_sem.at[g])

    for a in range(0, block, 2):
        result = lag_dot(right, turned_pair(rows, mid, lag, parts, a // GROUP * GROUP, a % GROUP), len(parts))
        for k in range(2):
            for slot in range(SLOTS):
                part = result[slot * block:(slot + 1) * block, k * LAGS:(k + 1) * LAGS]
                part = (acc[slot, a + k] + part) * scales[slot]
                if slot == 0:
                    part = jnp.where(lax.broadcasted_iota(jnp.int32, part.shape, 0) > a + k, part, 0.0)
                staged[slot, a + k] = part.astype(jnp.bfloat16)
        if (a + 2) % GROUP == 0:
            write(a // GROUP).start()
    for g in range(block // GROUP):
        write(g).wait()


def correlate(parts, partner, counts, own, near, far, acc):
    segments, _, block, _ = own.shape
    vmem = pl.BlockSpec(memory_space=pltpu.VMEM)
    return pl.pallas_call(
        functools.partial(correlate_kernel, parts),
        in_specs=[pl.BlockSpec(memory_space=pltpu.SMEM)] * 2 + [vmem] * 5,
        out_specs=pl.BlockSpec(memory_space=pltpu.HBM),
        scratch_shapes=[
            pltpu.VMEM((SLOTS, block, block, LAGS), jnp.bfloat16),
            pltpu.VMEM((len(parts), SLOTS * block, 128), jnp.bfloat16),
            pltpu.VMEM((segments, PARTS, block, 128), jnp.float32),
            pltpu.VMEM((segments, block, 128), jnp.float32),
            pltpu.VMEM((4, LAGS, 128), jnp.bfloat16),
            pltpu.SemaphoreType.DMA((block // GROUP,)),
        ],
        out_shape=jax.ShapeDtypeStruct((1, SLOTS, block, block, LAGS), jnp.bfloat16),
        cost_estimate=pl.CostEstimate(
            flops=6 * block * block * LAGS * len(parts) * 128, bytes_accessed=6_000_000, transcendentals=0),
        compiler_params=pltpu.CompilerParams(vmem_limit_bytes=15 * 2**20),
        name="correlate",
    )(partner, counts, own, near, far, acc, lag_tables())


def on_device(raw_samples, partner, counts):
    width, pieces, stages = tile_plan(raw_samples.shape[0], raw_samples.shape[1])
    own, near, far, acc = exchange(raw_samples, counts, width, pieces, stages)
    return correlate(stages[-1][2], partner, counts, own, near, far, acc)


def solution(mesh):
    return jax.shard_map(
        on_device,
        mesh=mesh,
        in_specs=(P("groups", "row", None), P(("groups", "row"), None), P(("groups", "row"), None)),
        out_specs=P(("groups", "row"), None, None, None, None),
        check_vma=False,
    )
```
